32 devices in a mesh: expert: 8 (over z, x), row: 4 (over y, core).
Axes of the slice: x: 2, y: 2, z: 4, core: 2. Of those that a mesh axis runs over, the one named last changes fastest.
Arguments:
- momentum: bfloat16 [8, 3584, 2048], P('expert', 'row'), may hold values from -6 to 6
- gradient: bfloat16 [8, 3584, 2048], P('expert', 'row'), may hold values from -96 to 96
- basis: float32 [8, 2048, 512], P('expert', 'row'), may hold values from -0.125 to 0.125
- ranks: int32 [8], replicated, may hold values from 128 to 512, as said below
- assignment: int32 [8], replicated, may hold values from 0 to 7, each once
Outputs:
- new_momentum: bfloat16 [8, 3584, 2048], P('expert', 'row')
- update: bfloat16 [8, 3584, 2048], P('expert', 'row')
- new_basis: float32 [8, 2048, 512], P('expert', 'row')
The draws below stay inside these ranges and needn't reach their ends.
Inputs may be any that keep to these rules, and one draw needn't show every extreme that they name: `ranks`: some expert has rank 512 in every draw.
All inputs are finite; a program needn't handle non-finite values.
Results may differ from the reference program's by a relative error of at most 0.033.
Values may be sent and summed in bfloat16 or wider, within the bound.
No kernel may reach another device: no remote copies, remote signals or barrier semaphores. Data moves between devices by JAX's collectives and lax.ppermute only.
A program may use at most 64 MiB of HBM per device.

```python
import math
import jax
import jax.numpy as jnp
from jax import lax

ROWS = 3584
FF = 2048
RANK_MAX = 512
EXPERTS = 8


def draw_ranks(key, part):
    subkeys = jax.random.split(jax.random.fold_in(key, 11), 3)
    quarter = RANK_MAX // 4
    step_size = max(RANK_MAX // 16, 1)
    base_rank = quarter + step_size * jax.random.randint(subkeys[0], (EXPERTS,), 0, 4)
    heavy_rank = jax.random.randint(subkeys[1], (EXPERTS,), RANK_MAX // 2 + RANK_MAX // 4, RANK_MAX + 1)
    order_ids = jax.random.permutation(subkeys[2], EXPERTS)
    heavy_count = max(EXPERTS // 8, 1)
    rank_vals = jnp.where(order_ids < heavy_count, heavy_rank, base_rank)
    return jnp.where(order_ids == 0, RANK_MAX, rank_vals).astype(jnp.int32)


def draw_gradient(key, part):
    subkeys = jax.random.split(jax.random.fold_in(key, 23), 3)
    expert_pos = jnp.arange(EXPERTS, dtype=jnp.float32)
    expert_scale = 1.0 + 2.0 * expert_pos / max(EXPERTS - 1, 1)
    row_pos = jnp.arange(ROWS, dtype=jnp.float32)
    row_rise = 1.0 + 2.0 * row_pos / max(ROWS - 1, 1)
    block_ids = jnp.arange(ROWS, dtype=jnp.int32) * 16 // ROWS
    block_level = jnp.exp(jax.random.uniform(subkeys[2], (EXPERTS, 16), jnp.float32, -0.5, 0.5))
    row_level = row_rise[None, :] * block_level[:, block_ids]
    values = jnp.clip(jax.random.normal(subkeys[0], (EXPERTS, ROWS, FF), jnp.float32), -3.0, 3.0)
    values = values * row_level[:, :, None]
    return (values * expert_scale[:, None, None]).astype(jnp.bfloat16)


def block_scale(stream_key, shape, cuts, low, largest):
    gain = 1.0
    for position, blocks in cuts:
        heights = jax.random.uniform(jax.random.fold_in(jax.random.fold_in(stream_key, 6), position), (blocks,), jnp.float32, low / len(cuts), largest / len(cuts))
        gain = gain * jnp.repeat(jnp.exp(heights), shape[position] // blocks).reshape((-1,) + (1,) * (len(shape) - 1 - position))
    return gain


def noise(stream_key, extent, scale, bound, cuts=(), kind=jnp.bfloat16):
    gain = block_scale(stream_key, extent, cuts, -0.22, 0.18) if cuts else 1.0
    values = jax.random.normal(stream_key, extent, jnp.float32) * scale * gain
    return jnp.minimum(jnp.maximum(values, -bound), bound).astype(kind)


def setup_inputs(seed: int = 0) -> dict:
    seeds = jax.random.split(jax.random.key(seed), 6)
    return {
        "momentum": noise(seeds[0], (EXPERTS, ROWS, FF), 1.0, 6.0, ((0, 8), (1, 4))),
        "gradient": draw_gradient(jax.random.fold_in(seeds[5], 71), 0),
        "basis": noise(seeds[2], (EXPERTS, FF, RANK_MAX), FF ** -0.5, 0.125, ((0, 8), (1, 4)), jnp.float32),
        "ranks": draw_ranks(jax.random.fold_in(seeds[5], 71), 0),
        "assignment": jax.random.permutation(seeds[4], EXPERTS).astype(jnp.int32),
    }


epsilon = 1e-06
mu_decay = 0.9
clip_target = 0.5

def one_expert(items, clip_scale):
    mom_block, grad_block, basis_block, rank_now = items
    buffer_full = mom_block.astype(jnp.float32) + clip_scale * grad_block.astype(jnp.float32)
    buffer = buffer_full.astype(jnp.bfloat16)
    keep_mask = (jnp.arange(RANK_MAX, dtype=jnp.int32) < rank_now).astype(jnp.float32)
    basis_half = (basis_block * keep_mask[None, :]).astype(jnp.bfloat16)
    power_cols = jnp.dot(buffer.astype(jnp.float32), basis_half.astype(jnp.float32), preferred_element_type=jnp.float32)
    gram_sum = lax.dot_general(power_cols.astype(jnp.float32), power_cols.astype(jnp.float32), (((0,), (0,)), ((), ())), precision=lax.Precision.HIGHEST, preferred_element_type=jnp.float32)
    gram_sum = gram_sum * keep_mask[:, None] * keep_mask[None, :] + jnp.diag(1.0 - keep_mask)
    lower_factor = jnp.linalg.cholesky(gram_sum)
    identity = jnp.eye(RANK_MAX, dtype=jnp.float32)
    inverse = lax.linalg.triangular_solve(lower_factor, identity, left_side=True, lower=True)
    orthonormal = lax.dot_general(power_cols.astype(jnp.float32), inverse.astype(jnp.float32), (((1,), (1,)), ((), ())), precision=lax.Precision.HIGHEST, preferred_element_type=jnp.float32)
    ortho_half = orthonormal.astype(jnp.bfloat16)
    factor = lax.dot_general(buffer.astype(jnp.float32), ortho_half.astype(jnp.float32), (((0,), (0,)), ((), ())), preferred_element_type=jnp.float32)
    col_sq = lax.optimization_barrier(jnp.sum(factor * factor, axis=0))
    inv_norm = lax.rsqrt(col_sq + epsilon)
    new_basis = factor * inv_norm[None, :]
    factor_half = factor.astype(jnp.bfloat16)
    feedback = lax.dot_general(ortho_half.astype(jnp.float32), factor_half.astype(jnp.float32), (((1,), (1,)), ((), ())), preferred_element_type=jnp.float32)
    new_momentum = (buffer_full - (1.0 - mu_decay) * feedback).astype(jnp.bfloat16)
    update_gain = math.sqrt(ROWS * FF / RANK_MAX)
    scaled = (orthonormal * (inv_norm * update_gain)[None, :]).astype(jnp.bfloat16)
    update = lax.dot_general(scaled.astype(jnp.float32), factor_half.astype(jnp.float32), (((1,), (1,)), ((), ())), preferred_element_type=jnp.float32).astype(jnp.bfloat16)
    return (new_momentum, update, new_basis)

def reference(momentum, gradient, basis, ranks, assignment):
    sq_sums = lax.map(lambda block: jnp.sum(jnp.square(block.astype(jnp.float32))), gradient)
    mean_sq = jnp.sum(sq_sums) / (EXPERTS * ROWS * FF)
    clip_scale = jnp.minimum(1.0, clip_target * lax.rsqrt(mean_sq + epsilon))
    rank_groups = ranks[assignment]
    return lax.map(lambda items: one_expert(items, clip_scale), (momentum, gradient, basis, rank_groups))
```

```python
import functools
import math

import jax
import jax.numpy as jnp
from jax import lax
from jax.experimental import pallas as pl
from jax.experimental.pallas import tpu as pltpu
from jax.sharding import PartitionSpec as P

ROWS = 3584
FF = 2048
RANK_MAX = 512


epsilon = 1e-06
mu_decay = 0.9
clip_target = 0.5

HIGHEST = lax.Precision.HIGHEST
F32 = jnp.float32
BF16 = jnp.bfloat16


def mul_nt(a, b):
    return lax.dot_general(
        a, b, (((1,), (1,)), ((), ())), precision=HIGHEST, preferred_element_type=F32
    )


def mul_nn(a, b):
    return lax.dot_general(
        a, b, (((1,), (0,)), ((), ())), precision=HIGHEST, preferred_element_type=F32
    )


def small_inverse(a, n):
    tiles = n // 8
    sub = lax.broadcasted_iota(jnp.int32, (8, n), 0)
    lane = lax.broadcasted_iota(jnp.int32, (8, n), 1)
    cols = [
        [
            jnp.broadcast_to(a[8 * t : 8 * t + 8, c : c + 1], (8, n)) if t >= c // 8 else None
            for t in range(tiles)
        ]
        for c in range(n)
    ]
    inv = [(sub + 8 * t == lane).astype(F32) for t in range(tiles)]
    for c in range(n):
        top, s = divmod(c, 8)
        r = lax.rsqrt(jnp.broadcast_to(cols[c][top][s : s + 1, :], (8, n)))
        row = jnp.broadcast_to(inv[top][s : s + 1, :], (8, n)) * r
        mult = [cols[c][t] * r if t >= top else None for t in range(tiles)]
        mult[top] = jnp.where(sub > s, mult[top], 0.0)
        for d in range(c + 1, n):
            td, sd = divmod(d, 8)
            factor = jnp.broadcast_to(mult[td][sd : sd + 1, :], (8, n))
            for t in range(td, tiles):
                cols[d][t] = cols[d][t] - mult[t] * factor
        for t in range(top, tiles):
            new = inv[t] - mult[t] * row
            inv[t] = jnp.where(sub == s, row, new) if t == top else new
    return jnp.concatenate(inv, axis=0)


def block_inverse(a, n, b):
    k = n // b
    blk = [
        [a[i * b : (i + 1) * b, j * b : (j + 1) * b] if j <= i else None for j in range(k)]
        for i in range(k)
    ]
    low = [[None] * k for _ in range(k)]
    inv = [[None] * k for _ in range(k)]
    for j in range(k):
        inv[j][j] = small_inverse(blk[j][j], b)
        for i in range(j + 1, k):
            low[i][j] = mul_nt(blk[i][j], inv[j][j])
        for i in range(j + 1, k):
            for l in range(j + 1, i + 1):
                blk[i][l] = blk[i][l] - mul_nt(low[i][j], low[l][j])
        for l in range(j):
            acc = mul_nn(low[j][l], inv[l][l])
            for m in range(l + 1, j):
                acc = acc + mul_nn(low[j][m], inv[m][l])
            inv[j][l] = -mul_nn(inv[j][j], acc)
    zero = jnp.zeros((b, b), F32)
    return jnp.concatenate(
        [
            jnp.concatenate([inv[i][j] if j <= i else zero for j in range(k)], axis=1)
            for i in range(k)
        ],
        axis=0,
    )


def inverse_kernel(n, b, c, gram_ref, out_ref):
    out_ref[...] = jnp.zeros((n, n), F32)
    for j in range(n // b):
        o = j * b
        rows = gram_ref[o : o + b, :]
        diag = rows[:, o : o + b]
        if j:
            done = out_ref[:o, :o]
            low = mul_nt(rows[:, :o], done)
            diag = diag - mul_nt(low, low)
            carried = mul_nn(low, done)
        inv = block_inverse(diag, b, c)
        out_ref[o : o + b, o : o + b] = inv
        if j:
            out_ref[o : o + b, :o] = -mul_nn(inv, carried)


def factor_inverse(gram):
    n = gram.shape[0]
    return pl.pallas_call(
        functools.partial(inverse_kernel, n, 128, 32),
        out_shape=jax.ShapeDtypeStruct((n, n), F32),
        in_specs=[pl.BlockSpec(memory_space=pltpu.VMEM)],
        out_specs=pl.BlockSpec(memory_space=pltpu.VMEM),
        name="factor_inverse",
    )(gram)


def swap(x, axis, bit):
    size = lax.axis_size(axis)
    return lax.ppermute(x, axis, [(i, i ^ bit) for i in range(size)])


def bits(size, first=1):
    out = []
    while first < size:
        out.append(first)
        first *= 2
    return out


def total_of(x):
    for axis in ("row", "expert"):
        for bit in bits(lax.axis_size(axis)):
            x = x + swap(x, axis, bit)
    return x


def gather_rows(x):
    size = lax.axis_size("row")
    index = lax.axis_index("row")
    held = x[None]
    for bit in bits(size, 2):
        other = swap(held, "row", bit)
        low = (index & bit) == 0
        held = jnp.concatenate(
            [jnp.where(low, held, other), jnp.where(low, other, held)], axis=0
        )
    other = swap(held, "row", 1)
    low = (index & 1) == 0
    return jnp.stack([jnp.where(low, held, other), jnp.where(low, other, held)], axis=1).reshape(
        (size,) + x.shape
    )


def sum_half(x):
    core = lax.axis_index("row") & 1
    mine = lax.dynamic_index_in_dim(x, core, 1, keepdims=False)
    other = lax.dynamic_index_in_dim(x, 1 - core, 1, keepdims=False)
    part = mine + swap(other.astype(BF16), "row", 1).astype(F32)
    for bit in bits(lax.axis_size("row"), 2):
        sent = part.astype(BF16)
        part = sent.astype(F32) + swap(sent, "row", bit).astype(F32)
    return part


def join_halves(x):
    core = lax.axis_index("row") & 1
    other = swap(x, "row", 1)
    low = core == 0
    return jnp.stack([jnp.where(low, x, other), jnp.where(low, other, x)], axis=1)


def local(momentum, gradient, basis, ranks, assignment):
    momentum, gradient = momentum[0], gradient[0]
    rows, hidden = gradient.shape
    width = basis.shape[2]
    row_size = lax.axis_size("row")
    grad_full = gradient.astype(F32)
    total_sq = total_of(jnp.sum(grad_full * grad_full).reshape(1, 1))[0, 0]
    entry_count = float(rows * hidden * row_size * lax.axis_size("expert"))
    clip_scale = jnp.minimum(1.0, clip_target * lax.rsqrt(total_sq / entry_count + epsilon))

    group_index = lax.axis_index("expert")
    slot_ids = jnp.arange(assignment.shape[0], dtype=jnp.int32)
    expert_id = jnp.sum(jnp.where(slot_ids == group_index, assignment, 0))
    rank_now = jnp.sum(jnp.where(slot_ids == expert_id, ranks, 0))
    keep_mask = (jnp.arange(width, dtype=jnp.int32) < rank_now).astype(F32)
    basis_half = (basis[0] * keep_mask[None, :]).astype(BF16)
    basis_all = gather_rows(basis_half).reshape(hidden, width)

    power_mom = jnp.dot(momentum, basis_all, preferred_element_type=F32)
    power_grad = jnp.dot(gradient, basis_all, preferred_element_type=F32)
    power_cols = power_mom + clip_scale * power_grad
    gram_part = lax.dot_general(
        power_cols,
        power_cols,
        (((0,), (0,)), ((), ())),
        precision=HIGHEST,
        preferred_element_type=F32,
    )
    gram_half = sum_half(gram_part.reshape(1, 2, width // 2, width))
    gram_sum = join_halves(gram_half.astype(BF16)).reshape(width, width).astype(F32)
    gram_sum = gram_sum * keep_mask[:, None] * keep_mask[None, :] + jnp.diag(1.0 - keep_mask)
    inverse = factor_inverse(gram_sum)

    buffer_full = momentum.astype(F32) + clip_scale * grad_full
    buffer = buffer_full.astype(BF16)
    orthonormal = lax.dot_general(
        power_cols,
        inverse,
        (((1,), (1,)), ((), ())),
        precision=HIGHEST,
        preferred_element_type=F32,
    )
    ortho_half = orthonormal.astype(BF16)
    factor_part = lax.dot_general(
        buffer, ortho_half, (((0,), (0,)), ((), ())), preferred_element_type=F32
    )
    block = hidden // row_size
    factor_own = sum_half(factor_part.reshape(row_size // 2, 2, block, width))
    factor_half = join_halves(factor_own.astype(BF16)).reshape(hidden, width)
    wide = factor_half.astype(F32)
    inv_norm = lax.rsqrt(jnp.sum(wide * wide, axis=0) + epsilon)
    own_rows = lax.dynamic_index_in_dim(factor_own, lax.axis_index("row") // 2, 0, keepdims=False)
    new_basis = own_rows * inv_norm[None, :]
    feedback = lax.dot_general(
        ortho_half, factor_half, (((1,), (1,)), ((), ())), preferred_element_type=F32
    )
    new_momentum = (buffer_full - (1.0 - mu_decay) * feedback).astype(BF16)
    update_gain = math.sqrt(ROWS * FF / RANK_MAX)
    scaled = (orthonormal * (inv_norm * update_gain)[None, :]).astype(BF16)
    update = lax.dot_general(
        scaled, factor_half, (((1,), (1,)), ((), ())), preferred_element_type=F32
    ).astype(BF16)
    return (new_momentum[None], update[None], new_basis[None])


def solution(mesh):
    placed = (
        P("expert", "row", None),
        P("expert", "row", None),
        P("expert", "row", None),
        P(),
        P(),
    )
    return jax.shard_map(
        local,
        mesh=mesh,
        in_specs=placed,
        out_specs=(P("expert", "row", None), P("expert", "row", None), P("expert", "row", None)),
        check_vma=False,
    )
```

```python
import functools
import math

import jax
import jax.numpy as jnp
from jax import lax
from jax.experimental import pallas as pl
from jax.experimental.pallas import tpu as pltpu
from jax.sharding import PartitionSpec as P


epsilon = 1e-06
mu_decay = 0.9
clip_target = 0.5

HIGHEST = lax.Precision.HIGHEST
F32 = jnp.float32
BF16 = jnp.bfloat16


def mul_nt(a, b):
    return lax.dot_general(
        a, b, (((1,), (1,)), ((), ())), precision=HIGHEST, preferred_element_type=F32
    )


def mul_nn(a, b):
    return lax.dot_general(
        a, b, (((1,), (0,)), ((), ())), precision=HIGHEST, preferred_element_type=F32
    )


def small_inverse(a, n):
    tiles = n // 8
    sub = lax.broadcasted_iota(jnp.int32, (8, n), 0)
    lane = lax.broadcasted_iota(jnp.int32, (8, n), 1)
    cols = [
        [
            jnp.broadcast_to(a[8 * t : 8 * t + 8, c : c + 1], (8, n)) if t >= c // 8 else None
            for t in range(tiles)
        ]
        for c in range(n)
    ]
    inv = [(sub + 8 * t == lane).astype(F32) for t in range(tiles)]
    for c in range(n):
        top, s = divmod(c, 8)
        r = lax.rsqrt(jnp.broadcast_to(cols[c][top][s : s + 1, :], (8, n)))
        row = jnp.broadcast_to(inv[top][s : s + 1, :], (8, n)) * r
        mult = [cols[c][t] * r if t >= top else None for t in range(tiles)]
        mult[top] = jnp.where(sub > s, mult[top], 0.0)
        for d in range(c + 1, n):
            td, sd = divmod(d, 8)
            factor = jnp.broadcast_to(mult[td][sd : sd + 1, :], (8, n))
            for t in range(td, tiles):
                cols[d][t] = cols[d][t] - mult[t] * factor
        for t in range(top, tiles):
            new = inv[t] - mult[t] * row
            inv[t] = jnp.where(sub == s, row, new) if t == top else new
    return jnp.concatenate(inv, axis=0)


def block_inverse(a, n, b):
    k = n // b
    blk = [
        [a[i * b : (i + 1) * b, j * b : (j + 1) * b] if j <= i else None for j in range(k)]
        for i in range(k)
    ]
    low = [[None] * k for _ in range(k)]
    inv = [[None] * k for _ in range(k)]
    for j in range(k):
        inv[j][j] = small_inverse(blk[j][j], b)
        for i in range(j + 1, k):
            low[i][j] = mul_nt(blk[i][j], inv[j][j])
        for i in range(j + 1, k):
            for l in range(j + 1, i + 1):
                blk[i][l] = blk[i][l] - mul_nt(low[i][j], low[l][j])
        for l in range(j):
            acc = mul_nn(low[j][l], inv[l][l])
            for m in range(l + 1, j):
                acc = acc + mul_nn(low[j][m], inv[m][l])
            inv[j][l] = -mul_nn(inv[j][j], acc)
    zero = jnp.zeros((b, b), F32)
    return jnp.concatenate(
        [
            jnp.concatenate([inv[i][j] if j <= i else zero for j in range(k)], axis=1)
            for i in range(k)
        ],
        axis=0,
    )


def lower_blocks(k):
    return [(i, j) for i in range(k) for j in range(i + 1)]


def keep_of(rank, shape, axis):
    return (lax.broadcasted_iota(jnp.int32, shape, axis) < rank).astype(F32)


def rank_of(place_ref, ranks_ref, assignment_ref):
    return ranks_ref[assignment_ref[place_ref[0]]]


def split(x):
    high = x.astype(BF16)
    return high, (x - high.astype(F32)).astype(BF16)


def dot_nn(a, b):
    return lax.dot_general(a, b, (((1,), (0,)), ((), ())), preferred_element_type=F32)


def dot_nt(a, b):
    return lax.dot_general(a, b, (((1,), (1,)), ((), ())), preferred_element_type=F32)


def scale_of(sums, entry_count):
    total = jnp.sum(sums, keepdims=True).reshape(1, 1)
    return jnp.minimum(1.0, clip_target * lax.rsqrt(total / entry_count + epsilon))


def mask_kernel(place_ref, ranks_ref, assignment_ref, basis_ref, out_ref):
    rank = rank_of(place_ref, ranks_ref, assignment_ref)
    out_ref[...] = (basis_ref[...] * keep_of(rank, (1, basis_ref.shape[1]), 1)).astype(BF16)


def power_kernel(count, entry_count, b, place_ref, sums_ref, mom_ref, grad_ref, *rest):
    parts = rest[:count]
    buffer_ref, high_ref, low_ref, thigh_ref, tlow_ref, gram_ref, acc_ref = rest[count:]
    step = pl.program_id(0)
    scale = scale_of(sums_ref[...], entry_count)
    buffer = (mom_ref[...].astype(F32) + scale * grad_ref[...].astype(F32)).astype(BF16)
    buffer_ref[...] = buffer

    for k in range(count):

        @pl.when(step == k)
        def _(k=k):
            add = dot_nn(buffer, parts[k][...])
            acc_ref[...] = add if k == 0 else acc_ref[...] + add

    @pl.when(step == count - 1)
    def _():
        power = acc_ref[...]
        high, low = split(power)
        high_ref[...] = high
        low_ref[...] = low
        thigh, tlow = split(power.T)
        thigh_ref[...] = thigh
        tlow_ref[...] = tlow
        blocks = lower_blocks(power.shape[1] // b)
        half = len(blocks) // 2
        for j in range(power.shape[1] // b):
            col = slice(j * b, (j + 1) * b)
            below = slice(j * b, power.shape[1])
            gram = (
                dot_nn(thigh[below], high[:, col])
                + dot_nn(thigh[below], low[:, col])
                + dot_nn(tlow[below], high[:, col])
            ).astype(BF16)
            for i in range(j, power.shape[1] // b):
                at = blocks.index((i, j))
                gram_ref[at // half, at % half] = gram[(i - j) * b : (i - j + 1) * b]


def power_and_gram(place, sums, momentum, gradient, parts, entry_count, b):
    rows, hidden = momentum.shape
    block, width = parts[0].shape
    count = len(parts)
    pairs = len(lower_blocks(width // b))
    moving = pl.BlockSpec((rows, block), lambda k, place: (0, place[1] ^ k))
    whole = pl.BlockSpec(memory_space=pltpu.VMEM)
    return pl.pallas_call(
        functools.partial(power_kernel, count, entry_count, b),
        grid_spec=pltpu.PrefetchScalarGridSpec(
            num_scalar_prefetch=1,
            grid=(count,),
            in_specs=[whole, moving, moving] + [whole] * count,
            out_specs=[moving] + [whole] * 5,
            scratch_shapes=[pltpu.VMEM((rows, width), F32)],
        ),
        out_shape=[
            jax.ShapeDtypeStruct((rows, hidden), BF16),
            jax.ShapeDtypeStruct((rows, width), BF16),
            jax.ShapeDtypeStruct((rows, width), BF16),
            jax.ShapeDtypeStruct((width, rows), BF16),
            jax.ShapeDtypeStruct((width, rows), BF16),
            jax.ShapeDtypeStruct((2, pairs // 2, b, b), BF16),
        ],
        name="power_and_gram",
    )(place, sums, momentum, gradient, *parts)


def cross_kernel(block, chips, thigh_ref, tlow_ref, buffer_ref, out_ref):
    for core in range(2):
        for chip in range(chips):
            at = (2 * chip + core) * block
            cols = buffer_ref[:, at : at + block]
            out_ref[core, chip] = (
                dot_nn(thigh_ref[...], cols) + dot_nn(tlow_ref[...], cols)
            ).astype(BF16)


def cross_product(thigh, tlow, buffer, block):
    width = thigh.shape[0]
    chips = buffer.shape[1] // block // 2
    whole = pl.BlockSpec(memory_space=pltpu.VMEM)
    return pl.pallas_call(
        functools.partial(cross_kernel, block, chips),
        out_shape=jax.ShapeDtypeStruct((2, chips, width, block), BF16),
        in_specs=[whole] * 3,
        out_specs=whole,
        name="cross_product",
    )(thigh, tlow, buffer)


def inverse_kernel(n, b, c, place_ref, ranks_ref, assignment_ref, gram_ref, out_ref):
    rank = rank_of(place_ref, ranks_ref, assignment_ref)
    blocks = lower_blocks(n // b)
    out_ref[...] = jnp.zeros((n, n), F32)

    def gram_block(i, j):
        kept = keep_of(rank - i * b, (b, 1), 0) * keep_of(rank - j * b, (1, b), 1)
        value = gram_ref[blocks.index((i, j))].astype(F32) * kept
        if i == j:
            row = lax.broadcasted_iota(jnp.int32, (b, b), 0)
            col = lax.broadcasted_iota(jnp.int32, (b, b), 1)
            value = value + jnp.where((row == col) & (row >= rank - i * b), 1.0, 0.0)
        return value

    for j in range(n // b):
        o = j * b
        diag = gram_block(j, j)
        if j:
            done = out_ref[:o, :o]
            left = jnp.concatenate([gram_block(j, i) for i in range(j)], axis=1)
            low = mul_nt(left, done)
            diag = diag - mul_nt(low, low)
            carried = mul_nn(low, done)
        inv = block_inverse(diag, b, c)
        out_ref[o : o + b, o : o + b] = inv
        if j:
            out_ref[o : o + b, :o] = -mul_nn(inv, carried)


def factor_inverse(place, ranks, assignment, gram, n, b):
    scalar = pl.BlockSpec(memory_space=pltpu.SMEM)
    whole = pl.BlockSpec(memory_space=pltpu.VMEM)
    return pl.pallas_call(
        functools.partial(inverse_kernel, n, b, 32),
        out_shape=jax.ShapeDtypeStruct((n, n), F32),
        in_specs=[scalar, scalar, scalar, whole],
        out_specs=whole,
        name="factor_inverse",
    )(place, ranks, assignment, gram)


def final_kernel(
    entry_count, gain, place_ref, sums_ref, inv_ref, high_ref, low_ref, cross_ref,
    mom_ref, grad_ref, new_mom_ref, update_ref, new_basis_ref, ortho_ref, fact_ref, scaled_ref
):
    step = pl.program_id(0)
    chips = cross_ref.shape[1]

    @pl.when(step == 0)
    def _():
        whigh, wlow = split(inv_ref[...])
        ortho_ref[...] = (
            dot_nt(high_ref[...], whigh) + dot_nt(high_ref[...], wlow) + dot_nt(low_ref[...], whigh)
        ).astype(BF16)
        squares = jnp.zeros((inv_ref.shape[0], 1), F32)
        for chip in range(chips):
            for core in range(2):
                at = 2 * chip + core
                cols = cross_ref[core, chip]
                fact = dot_nn(whigh, cols) + dot_nn(wlow, cols)
                squares = squares + jnp.sum(fact * fact, axis=1, keepdims=True)
                fact_ref[at] = fact
        inv_norm = lax.rsqrt(squares + epsilon)
        mine = place_ref[1]
        new_basis_ref[...] = (fact_ref[mine] * inv_norm).T
        for at in range(2 * chips):
            scaled_ref[at] = (fact_ref[at] * (inv_norm * gain)).astype(BF16)

    scale = scale_of(sums_ref[...], entry_count)
    ortho = ortho_ref[...]
    feedback = dot_nn(ortho, fact_ref[step].astype(BF16))
    buffer_full = mom_ref[...].astype(F32) + scale * grad_ref[...].astype(F32)
    new_mom_ref[...] = (buffer_full - (1.0 - mu_decay) * feedback).astype(BF16)
    update_ref[...] = dot_nn(ortho, scaled_ref[step]).astype(BF16)


def finish(place, sums, inverse, high, low, cross, momentum, gradient, entry_count, gain):
    rows, hidden = momentum.shape
    _, chips, width, block = cross.shape
    moving = pl.BlockSpec((rows, block), lambda k, place: (0, k))
    whole = pl.BlockSpec(memory_space=pltpu.VMEM)
    return pl.pallas_call(
        functools.partial(final_kernel, entry_count, gain),
        grid_spec=pltpu.PrefetchScalarGridSpec(
            num_scalar_prefetch=1,
            grid=(2 * chips,),
            in_specs=[whole] * 5 + [moving, moving],
            out_specs=[moving, moving, whole],
            scratch_shapes=[
                pltpu.VMEM((rows, width), BF16),
                pltpu.VMEM((2 * chips, width, block), F32),
                pltpu.VMEM((2 * chips, width, block), BF16),
            ],
        ),
        out_shape=[
            jax.ShapeDtypeStruct((rows, hidden), BF16),
            jax.ShapeDtypeStruct((rows, hidden), BF16),
            jax.ShapeDtypeStruct((block, width), F32),
        ],
        name="finish",
    )(place, sums, inverse, high, low, cross, momentum, gradient)


def swap(x, bit):
    size = lax.axis_size("row")
    return lax.ppermute(x, "row", [(i, i ^ bit) for i in range(size)])


def sum_half(x):
    core = lax.axis_index("row") & 1
    mine = lax.dynamic_index_in_dim(x, core, 0, keepdims=False)
    other = lax.dynamic_index_in_dim(x, 1 - core, 0, keepdims=False)
    arrived = swap(other, 1)
    part = mine.astype(F32) + arrived.astype(F32)
    bit = 2
    while bit < lax.axis_size("row"):
        sent = part.astype(BF16)
        arrived = swap(sent, bit)
        part = sent.astype(F32) + arrived.astype(F32)
        bit *= 2
    return part.astype(BF16)


def join_halves(x):
    core = lax.axis_index("row") & 1
    other = swap(x, 1)
    low = core == 0
    return jnp.stack([jnp.where(low, x, other), jnp.where(low, other, x)], axis=0)


def step(momentum, gradient, basis, ranks, assignment):
    momentum, gradient = momentum[0], gradient[0]
    rows, hidden = gradient.shape
    block, width = basis.shape[1:]
    row_size, groups = lax.axis_size("row"), lax.axis_size("expert")
    entry_count = float(rows * hidden * row_size * groups)
    b = 128
    place = jnp.stack([lax.axis_index("expert"), lax.axis_index("row")]).astype(jnp.int32)
    scalar = pl.BlockSpec(memory_space=pltpu.SMEM)
    whole = pl.BlockSpec(memory_space=pltpu.VMEM)

    basis_half = pl.pallas_call(
        mask_kernel,
        out_shape=jax.ShapeDtypeStruct((block, width), BF16),
        in_specs=[scalar, scalar, scalar, whole],
        out_specs=whole,
        name="mask",
    )(place, ranks, assignment, basis[0])

    chips = row_size // 2
    across = [basis_half] + [swap(basis_half, 2 * k) for k in range(1, chips)]
    grad_full = gradient.astype(F32)
    sums = jnp.sum((grad_full * grad_full).reshape(-1, 8, hidden), axis=0)
    sums = jnp.sum(jnp.sum(sums, axis=0).reshape(hidden // 128, 128), axis=0)
    everyone = row_size * groups
    sums = lax.all_to_all(
        jnp.broadcast_to(sums[None], (everyone, 128)), ("expert", "row"), 0, 0, tiled=True
    )
    parts = []
    for one in across:
        parts += [one, swap(one, 1)]

    buffer, high, low, thigh, tlow, gram = power_and_gram(
        place, sums, momentum, gradient, parts, entry_count, b
    )
    gram_half = sum_half(gram)
    cross = cross_product(thigh, tlow, buffer, block)
    cross = sum_half(cross)
    gram_sum = join_halves(gram_half).reshape(-1, b, b)
    inverse = factor_inverse(place, ranks, assignment, gram_sum, width, b)
    cross = join_halves(cross)
    gain = math.sqrt(rows * row_size * hidden / width)
    new_momentum, update, new_basis = finish(
        place, sums, inverse, high, low, cross, momentum, gradient, entry_count, gain
    )
    return (new_momentum[None], update[None], new_basis[None])


def solution(mesh):
    placed = (
        P("expert", "row", None),
        P("expert", "row", None),
        P("expert", "row", None),
        P(),
        P(),
    )
    return jax.shard_map(
        step,
        mesh=mesh,
        in_specs=placed,
        out_specs=(P("expert", "row", None), P("expert", "row", None), P("expert", "row", None)),
        check_vma=False,
    )
```
